256 devices in a mesh: lat: 32 (over y, x, core), lev: 8 (over z).
Axes of the slice: x: 4, y: 4, z: 8, core: 2. Of those that a mesh axis runs over, the one named last changes fastest.
Arguments:
- fields: float32 [12, 128, 256, 1024], P(None, 'lev', 'lat'), may hold values from -6 to 6
- legendre: bfloat16 [256, 256, 256], P('lat'), as said below
- owner_counts: int32 [32], replicated, may hold values from 1 to 16, 256 in all
Outputs:
- covariance: float32 [512, 128, 128], P('lat', 'lev')
The draws below stay inside these ranges and needn't reach their ends.
Inputs may be any that keep to these rules, and one draw needn't show every extreme that they name: `owner_counts`: each owner holds 1 to 16 total wavenumbers, the counts sum to 256, and some owner holds exactly 16. legendre[lat, m, n] is zero where n < m.
All inputs are finite; a program needn't handle non-finite values.
Results may differ from the reference program's by a relative error of at most 0.0038.
Values may be sent and summed in bfloat16 or wider, within the bound.
A program may use at most 128 MiB of HBM per device.

```python
import math
import jax
import jax.numpy as jnp
import numpy as np
from jax import lax

NLON = 1024
NLAT = 256
MTRUNC = 256
LEV = 128
MEM = 12
NCAP = 16
OWNERS = 32


def draw_legendre(key, part):
    values = jax.random.normal(key, (NLAT, MTRUNC, MTRUNC), jnp.float32) * NLAT ** (-0.5)
    order = jnp.arange(MTRUNC, dtype=jnp.int32)
    keeper = order[None, :] >= order[:, None]
    return jnp.where(keeper[None, :, :], values, jnp.zeros_like(values)).astype(jnp.bfloat16)


def levels(key, extent, shards, smallest, top_value):
    level = 1.0
    for position, parts in shards:
        draws = jax.random.uniform(jax.random.fold_in(jax.random.fold_in(key, 6), position), (parts,), jnp.float32, smallest / len(shards), top_value / len(shards))
        level = level * jnp.repeat(jnp.exp(draws), extent[position] // parts).reshape((-1,) + (1,) * (len(extent) - 1 - position))
    return level


def split_up(number_of, total, reach, slope):
    portions = [(1 << 20) // math.isqrt(rank ** slope) + 1 for rank in range(2, number_of + 1)]
    rest, given = total - reach - (number_of - 1), [1] * (number_of - 1)
    while rest > 0:
        candidates = [i for i in range(number_of - 1) if given[i] < reach]
        mass, remaining = sum([portions[i] for i in candidates]), rest
        for i in candidates:
            addition = min(reach - given[i], max(1, remaining * portions[i] // mass), rest)
            given[i] = given[i] + addition
            rest = rest - addition
    return np.array([reach] + given)


def ragged_sizes(key, number_of, total, most, skew):
    if number_of == 2:
        one = jax.random.randint(key, (), max(1, total - most), min(most, total - 1) + 1)
        return jnp.stack([one, total - one])
    lengths = jnp.asarray(split_up(number_of, total, most, skew), jnp.int32)
    couples = (number_of - 1) // 2
    giver, taker = lengths[1:1 + 2 * couples:2], lengths[2:2 + 2 * couples:2]
    room = jnp.minimum(giver - 1, most - taker)
    moved = jax.random.randint(jax.random.fold_in(key, 1), (couples,), 0, 1 << 20) % (room + 1)
    lengths = lengths.at[1:1 + 2 * couples:2].set(giver - moved).at[2:2 + 2 * couples:2].set(taker + moved)
    return lengths[jax.random.permutation(jax.random.fold_in(key, 2), number_of)]


def normal_values(key, shape, scale, most, split=(), kind=jnp.bfloat16):
    factor_of = levels(key, shape, split, -0.22, 0.18) if split else 1.0
    entries = jax.random.normal(key, shape, jnp.float32) * scale * factor_of
    return jnp.minimum(jnp.maximum(entries, -most), most).astype(kind)


def setup_inputs(seed: int = 0) -> dict:
    splits = jax.random.split(jax.random.key(seed), 4)
    return {
        "fields": normal_values(splits[0], (MEM, LEV, NLAT, NLON), 1.0, 6.0, ((1, 8), (2, 32)), jnp.float32),
        "legendre": draw_legendre(jax.random.fold_in(splits[3], 71), 0),
        "owner_counts": ragged_sizes(splits[2], OWNERS, MTRUNC, NCAP, 2).astype(jnp.int32),
    }


def reference(fields, legendre, owner_counts):
    transform = jnp.fft.rfft(fields, axis=-1)[..., :MTRUNC] * (NLON ** -0.5)
    stacked = jnp.stack([jnp.real(transform), jnp.imag(transform)], axis=0).astype(jnp.float32)
    spectra = jnp.transpose(stacked, (3, 4, 0, 1, 2)).astype(jnp.bfloat16)
    block_size = 32

    def add_block(running, block_id):
        spec_block = lax.dynamic_slice_in_dim(spectra, block_id * block_size, block_size, 1).astype(jnp.float32)
        transform_table_block = lax.dynamic_slice_in_dim(legendre, block_id * block_size, block_size, 1).astype(jnp.float32)
        wavenumber_rows = jnp.einsum('lmqbe,lmn->nmqbe', spec_block, transform_table_block)
        anomaly = (wavenumber_rows - jnp.mean(wavenumber_rows, axis=3, keepdims=True)).astype(jnp.bfloat16)
        anomaly = lax.optimization_barrier(anomaly).astype(jnp.float32)
        return running + jnp.einsum('nmqbe,nmqbk->nek', anomaly, anomaly), None

    blocks_all = jnp.arange(MTRUNC // block_size, dtype=jnp.int32)
    start_sum = jnp.zeros((MTRUNC, LEV, LEV), jnp.float32)
    full, unused = lax.scan(add_block, start_sum, blocks_all)
    wavenumber = jnp.arange(MTRUNC, dtype=jnp.int32)
    divisor = ((MEM - 1) * (2 * wavenumber + 2)).astype(jnp.float32)
    full = full / divisor[:, None, None]
    starts = (jnp.cumsum(owner_counts) - owner_counts).astype(jnp.int32)
    offset = jnp.arange(NCAP, dtype=jnp.int32)
    active_flag = offset[None, :] < owner_counts[:, None]
    slot_index = jnp.where(active_flag, starts[:, None] + offset[None, :], 0).reshape(-1).astype(jnp.int32)
    selected_entries = jnp.take(full, slot_index, axis=0)
    return jnp.where(active_flag.reshape(-1)[:, None, None], selected_entries, jnp.zeros_like(selected_entries))
```

```python
import functools

import jax
import jax.numpy as jnp
import numpy as np
from jax import lax
from jax.experimental import pallas as pl
from jax.experimental.pallas import tpu as pltpu
from jax.sharding import PartitionSpec as P

MESH = pl.DeviceIdType.MESH
F32, BF16 = jnp.float32, jnp.bfloat16
PAIRS = ((0, 4), (1, 7), (2, 6), (3, 5))
UNITS = 5
UNIT_ORDER = (0, 4, 1, 2, 3)


def peer(me, k):
    chip, core = k // 2, k % 2
    dx = chip % 4
    dy = (chip // 4 + dx) % 4
    return ((me // 8 + dy) % 4) * 8 + ((me // 2 + dx) % 4) * 2 + (me + core) % 2


def kernel(
    spec, leg, counts, out,
    leg_out, leg_in, spec_in, packed, waves, anom_out, anom_in, mixed, swapped, part_out, part_in, cov, own_out, own_in,
    send_sem, recv_sem,
):
    me, zed = lax.axis_index("lat"), lax.axis_index("lev")
    lats, levs = 32, 8
    share = lats // levs
    sem_l, sem_s, sem_a, sem_z, sem_p, sem_o = 0, 1, 5, 10, 15, 16

    barrier = pltpu.get_barrier_semaphore()

    @pl.loop(1, lats)
    def _(k):
        pl.semaphore_signal(barrier, inc=1, device_id={"lat": peer(me, k)}, device_id_type=MESH)

    @pl.loop(1, levs)
    def _(k):
        pl.semaphore_signal(barrier, inc=1, device_id={"lev": (zed + k) % levs}, device_id_type=MESH)

    def over_lat(source, target, sem):
        @pl.loop(1, lats)
        def _(k):
            to = peer(me, k)
            pltpu.make_async_remote_copy(
                source.at[to], target.at[me], send_sem.at[sem], recv_sem.at[sem],
                device_id={"lat": to}, device_id_type=MESH,
            ).start()

        target[me] = source[me]

    def lat_copy(source, target, sem):
        return pltpu.make_async_remote_copy(
            source.at[pl.ds(0, lats - 1)], target.at[pl.ds(0, lats - 1)], send_sem.at[sem], recv_sem.at[sem],
            device_id={"lat": peer(me, 1)}, device_id_type=MESH,
        )

    column = lax.broadcasted_iota(jnp.int32, (32, 256), 1)
    for u in range(UNITS):
        for j in range(8):
            rows = leg[j, 32 * u : 32 * u + 32, :].astype(F32)
            if 0 < u < 4:
                other = leg[j, 32 * (8 - u) : 32 * (8 - u) + 32, :].astype(F32)
                rows = jnp.where(column < 32 * u, pltpu.roll(other, 32 * u, 1), rows)
            elif u == 4:
                rows = jnp.where(column < 128, 0.0, rows)
            for c in range(2):
                packed[c, pl.ds(j, 32, stride=8), :] = rows[:, 128 * c : 128 * c + 128]
        for c in range(2):
            leg_out[:, u, :, 128 * c : 128 * c + 128] = packed[c].astype(BF16).reshape(32, 8, 128)

    pl.semaphore_wait(barrier, lats - 1 + levs - 1)
    over_lat(leg_out, leg_in, sem_l)
    for g in range(4):
        over_lat(spec.at[g], spec_in.at[g], sem_s + g)
    lat_copy(leg_out, leg_in, sem_l).wait_recv()

    def transform(u, g, aa):
        return lax.dot_general(
            leg_in[:, u].reshape(256, 256), spec_in[g, :, aa].reshape(256, 384),
            (((0,), (0,)), ((), ())), preferred_element_type=F32,
        )

    def keep(value, low, high):
        for c in range(3):
            waves[c, low:high, :] = value[low:high, 128 * c : 128 * c + 128]

    def send_anomalies(u):
        @pl.loop(0, lats, unroll=4)
        def _(i):
            for c in range(3):
                anom_out[u, i, :, 128 * c : 128 * c + 128] = waves[c, pl.ds(i, 8, stride=32), :].astype(BF16)

        over_lat(anom_out.at[u], anom_in.at[u], sem_a + u)

    def lev_copy(u, to):
        return pltpu.make_async_remote_copy(
            anom_in.at[u, pl.ds(share * to, share)], mixed.at[u, zed], send_sem.at[sem_z + u], recv_sem.at[sem_z + u],
            device_id={"lev": to}, device_id_type=MESH,
        )

    def over_lev(u):
        lat_copy(anom_out.at[u], anom_in.at[u], sem_a + u).wait_recv()

        @pl.loop(1, levs)
        def _(k):
            lev_copy(u, (zed + k) % levs).start()

        mixed[u, zed] = anom_in[u, pl.ds(share * zed, share)]

    def lev_wait(u):
        return pltpu.make_async_remote_copy(
            mixed.at[u, pl.ds(0, levs - 1)], mixed.at[u, pl.ds(0, levs - 1)], send_sem.at[sem_z + u], recv_sem.at[sem_z + u],
            device_id={"lev": (zed + 1) % levs}, device_id_type=MESH,
        )

    for g in range(4):
        lat_copy(spec.at[g], spec_in.at[g], sem_s + g).wait_recv()
        if g == 0:
            keep(transform(0, 0, 0), 0, 256)
            send_anomalies(0)
            keep(transform(4, 0, 1), 0, 256)
            send_anomalies(4)
        else:
            keep(transform(g, g, 0), 32 * g, 256)
            keep(transform(g, g, 1), 0, 32 * g)
            send_anomalies(g)
        if g == 1:
            over_lev(0)
            over_lev(4)
        elif g > 1:
            over_lev(g - 1)
    over_lev(3)

    group = lax.broadcasted_iota(jnp.int32, (32, 128), 1) // 16
    for u in UNIT_ORDER:
        lev_wait(u).wait_recv()
        for j in range(3):
            v = [mixed[u, z, :, :, 128 * j : 128 * j + 128].astype(F32).reshape(32, 128) for z in range(8)]
            for bit in (1, 2, 4):
                high = (group // bit) % 2 == 1
                w = list(v)
                for i in range(8):
                    if i // bit % 2 == 0:
                        w[i] = jnp.where(high, pltpu.roll(v[i + bit], 16 * bit, 1), v[i])
                        w[i + bit] = jnp.where(high, v[i + bit], pltpu.roll(v[i], 128 - 16 * bit, 1))
                v = w
            for x in range(8):
                swapped[pl.ds(((u * 3 + j) * 8 + x) * 32, 32), :] = v[x]

    for b in range(8):
        rows = [(u, b) for u in range(min(b, 4) + 1)] + [(u, b - 8 + u) for u in range(max(1, 8 - b), 4)]
        x = jnp.concatenate([swapped[pl.ds(u * 768 + r, 96, stride=8), :] for u, r in rows], axis=0).astype(BF16)
        gram = lax.dot_general(x, x, (((0,), (0,)), ((), ())), preferred_element_type=F32)
        part_out[:, b] = gram.astype(BF16).reshape(8, 16, 128)

    @pl.loop(1, levs)
    def _(k):
        to = (zed + k) % levs
        pltpu.make_async_remote_copy(
            part_out.at[to], part_in.at[zed], send_sem.at[sem_p], recv_sem.at[sem_p],
            device_id={"lev": to}, device_id_type=MESH,
        ).start()

    part_in[zed] = part_out[zed]
    part_wait = pltpu.make_async_remote_copy(
        part_out.at[pl.ds(0, levs - 1)], part_in.at[pl.ds(0, levs - 1)], send_sem.at[sem_p], recv_sem.at[sem_p],
        device_id={"lev": (zed + 1) % levs}, device_id_type=MESH,
    )
    part_wait.wait_recv()
    for b in range(8):
        total = part_in[0, b].astype(F32)
        for z in range(1, 8):
            total += part_in[z, b].astype(F32)
        cov[b] = total / (11 * (2 * (32 * b + me) + 2)).astype(F32)

    def choose(d, start):
        n = start + (me + 512 - start) % 32
        own_out[d] = cov[jnp.minimum(n // 32, 7)]
        return start + counts[d]

    lax.fori_loop(0, lats, choose, jnp.int32(0))
    over_lat(own_out, own_in, sem_o)
    start = lax.fori_loop(0, lats, lambda d, t: t + jnp.where(d < me, counts[d], 0), jnp.int32(0))
    live = jnp.broadcast_to(counts[me], (16, 128))
    lat_copy(own_out, own_in, sem_o).wait_recv()
    for j in range(16):
        value = own_in[(start + j) % 32]
        out[j] = jnp.where(live > j, value, 0.0)

    lat_copy(leg_out, leg_in, sem_l).wait_send()
    for g in range(4):
        lat_copy(spec.at[g], spec_in.at[g], sem_s + g).wait_send()
    for u in range(UNITS):
        lat_copy(anom_out.at[u], anom_in.at[u], sem_a + u).wait_send()
        lev_wait(u).wait_send()
    part_wait.wait_send()
    lat_copy(own_out, own_in, sem_o).wait_send()


def fourier_tables():
    x = np.arange(512)
    a = np.array([a for pair in PAIRS for a in pair])
    tables = []
    for parity in range(2):
        m = 32 * a[:, None] + 2 * np.arange(16)[None, :] + parity
        angle = 2.0 * np.pi * ((x[:, None, None] * m[None]) % 1024) / 1024
        tables.append(np.stack([np.cos(angle), -np.sin(angle)], axis=-1) / 32.0)
    return np.stack(tables).astype(np.float32)


def on_device(fields, legendre, owner_counts):
    centred = fields - jnp.mean(fields, axis=0, keepdims=True)
    first, second = centred[..., :512], centred[..., 512:]
    tables = fourier_tables()
    halves = [
        jnp.einsum("belx,xakq->aklqbe", x, tables[p], precision=lax.Precision.HIGH)
        for p, x in enumerate((first + second, first - second))
    ]
    spec = jnp.stack(halves, axis=2).astype(BF16).reshape(4, 2, 32, 8, 384)
    spec = jnp.moveaxis(spec, 1, 2)
    vmem = pl.BlockSpec(memory_space=pltpu.VMEM)
    return pl.pallas_call(
        kernel,
        out_shape=jax.ShapeDtypeStruct((16, 16, 128), F32),
        in_specs=[vmem, vmem, pl.BlockSpec(memory_space=pltpu.SMEM)],
        out_specs=vmem,
        scratch_shapes=[
            pltpu.VMEM((32, UNITS, 8, 256), BF16),
            pltpu.VMEM((32, UNITS, 8, 256), BF16),
            pltpu.VMEM((4, 32, 2, 8, 384), BF16),
            pltpu.VMEM((2, 256, 128), F32),
            pltpu.VMEM((3, 256, 128), F32),
            pltpu.VMEM((UNITS, 32, 8, 384), BF16),
            pltpu.VMEM((UNITS, 32, 8, 384), BF16),
            pltpu.VMEM((UNITS, 8, 4, 8, 384), BF16),
            pltpu.VMEM((UNITS * 768, 128), F32),
            pltpu.VMEM((8, 8, 16, 128), BF16),
            pltpu.VMEM((8, 8, 16, 128), BF16),
            pltpu.VMEM((8, 16, 128), F32),
            pltpu.VMEM((32, 16, 128), F32),
            pltpu.VMEM((32, 16, 128), F32),
            pltpu.SemaphoreType.DMA((17,)),
            pltpu.SemaphoreType.DMA((17,)),
        ],
        compiler_params=pltpu.CompilerParams(
            collective_id=0, has_side_effects=True, vmem_limit_bytes=48 * 2**20
        ),
        name="exchange",
    )(spec, legendre, owner_counts)


def solution(mesh):
    return jax.shard_map(
        on_device,
        mesh=mesh,
        in_specs=(P(None, "lev", "lat", None), P("lat", None, None), P()),
        out_specs=P("lat", "lev", None),
        check_vma=False,
    )
```

```python
import functools

import jax
import jax.numpy as jnp
import numpy as np
from jax import lax
from jax.experimental import pallas as pl
from jax.experimental.pallas import tpu as pltpu
from jax.sharding import PartitionSpec as P

MESH = pl.DeviceIdType.MESH
F32, BF16 = jnp.float32, jnp.bfloat16
PAIRS = ((0, 4), (1, 7), (2, 6), (3, 5))
UNITS = 5
UNIT_ORDER = (0, 4, 1, 2, 3)


def peer(me, k):
    chip, core = k // 2, k % 2
    dx = chip % 4
    dy = (chip // 4 + dx) % 4
    return ((me // 8 + dy) % 4) * 8 + ((me // 2 + dx) % 4) * 2 + (me + core) % 2


def centred(v):
    lane = lax.broadcasted_iota(jnp.int32, v[0].shape, 1)

    def whole(t):
        for shift in (64, 32, 16):
            t = t + pltpu.roll(t, shift, 1)
        return t

    t = v[1]
    for shift in (16, 32):
        t = t + jnp.where((lane // shift) % 2 == 0, pltpu.roll(t, 128 - shift, 1), pltpu.roll(t, shift, 1))
    other = pltpu.roll(t, 64, 1)
    real = (whole(v[0]) + jnp.where(lane < 64, t, other)) * (1.0 / 12.0)
    imag = (whole(v[2]) + jnp.where(lane < 64, other, t)) * (1.0 / 12.0)
    return v[0] - real, v[1] - jnp.where(lane < 64, real, imag), v[2] - imag


def kernel(
    fields, tables, leg, counts, out,
    grid, table, spectra, spec, leg_out, leg_in, spec_in, packed, waves, anom_out, anom_in, mixed, swapped, part_out, part_in, cov, own_out, own_in,
    send_sem, recv_sem, load_sem,
):
    me, zed = lax.axis_index("lat"), lax.axis_index("lev")
    lats, levs = 32, 8
    share = lats // levs
    sem_l, sem_s, sem_a, sem_z, sem_p, sem_o = 0, 1, 5, 10, 15, 16

    loads = [pltpu.make_async_copy(tables, table, load_sem.at[8])] + [
        pltpu.make_async_copy(fields.at[:, pl.ds(128 * c, 128)], grid.at[c], load_sem.at[c]) for c in range(8)
    ]
    for load in loads:
        load.start()
    barrier = pltpu.get_barrier_semaphore()

    @pl.loop(1, lats)
    def _(k):
        pl.semaphore_signal(barrier, inc=1, device_id={"lat": peer(me, k)}, device_id_type=MESH)

    @pl.loop(1, levs)
    def _(k):
        pl.semaphore_signal(barrier, inc=1, device_id={"lev": (zed + k) % levs}, device_id_type=MESH)

    def over_lat(source, target, sem, place=lambda to: to):
        @pl.loop(1, lats)
        def _(k):
            to = peer(me, k)
            pltpu.make_async_remote_copy(
                source.at[place(to)], target.at[me], send_sem.at[sem], recv_sem.at[sem],
                device_id={"lat": to}, device_id_type=MESH,
            ).start()

        target[me] = source[place(me)]

    def lat_copy(source, target, sem):
        return pltpu.make_async_remote_copy(
            source.at[pl.ds(0, lats - 1)], target.at[pl.ds(0, lats - 1)], send_sem.at[sem], recv_sem.at[sem],
            device_id={"lat": peer(me, 1)}, device_id_type=MESH,
        )

    column = lax.broadcasted_iota(jnp.int32, (32, 256), 1)
    for u in range(UNITS):
        for j in range(8):
            rows = leg[j, 32 * u : 32 * u + 32, :].astype(F32)
            if 0 < u < 4:
                other = leg[j, 32 * (8 - u) : 32 * (8 - u) + 32, :].astype(F32)
                rows = jnp.where(column < 32 * u, pltpu.roll(other, 32 * u, 1), rows)
            elif u == 4:
                rows = jnp.where(column < 128, 0.0, rows)
            for c in range(2):
                packed[c, pl.ds(j, 32, stride=8), :] = rows[:, 128 * c : 128 * c + 128]
        for c in range(2):
            leg_out[:, u, :, 128 * c : 128 * c + 128] = packed[c].astype(BF16).reshape(32, 8, 128)

    pl.semaphore_wait(barrier, lats - 1 + levs - 1)
    over_lat(leg_out, leg_in, sem_l)
    for load in loads:
        load.wait()

    lane = lax.broadcasted_iota(jnp.int32, (128, 128), 1)

    @pl.loop(0, 8)
    def _(j):
        for p in range(2):
            high, low = [], []
            for c in range(4):
                first = grid[c, pl.ds(j, 192, stride=8), :]
                second = grid[c + 4, pl.ds(j, 192, stride=8), :]
                value = first + second if p == 0 else first - second
                high.append(value.astype(BF16))
                low.append((value - high[-1].astype(F32)).astype(BF16))
            right = jnp.concatenate(high + low + high, axis=1)
            right = jnp.concatenate([right, jnp.zeros((64, 1536), BF16)], axis=0)
            left = jnp.concatenate([table[p, :, :512], table[p, :, :512], table[p, :, 512:]], axis=1)
            sums = lax.dot_general(left, right, (((1,), (1,)), ((), ())), preferred_element_type=F32)
            rows = pl.ds(1024 * p + j, 128, stride=8)
            spectra[0, rows, :] = sums[:128, :128]
            spectra[1, rows, :] = jnp.where(lane < 64, sums[:128, 128:], pltpu.roll(sums[128:, 128:], 64, 1))
            spectra[2, rows, :] = sums[128:, :128]

    for g in range(4):
        for aa in range(2):
            for p in range(2):
                for c in range(3):
                    value = spectra[c, pl.ds(1024 * p + 128 * (2 * g + aa), 128), :].astype(BF16)
                    spec[g, 16 * p : 16 * p + 16, aa, :, 128 * c : 128 * c + 128] = value.reshape(16, 8, 128)
        over_lat(spec.at[g], spec_in.at[g], sem_s + g, lambda to: 16 * (to % 2) + to // 2)
    lat_copy(leg_out, leg_in, sem_l).wait_recv()

    def transform(u, g, aa):
        return lax.dot_general(
            leg_in[:, u].reshape(256, 256), spec_in[g, :, aa].reshape(256, 384),
            (((0,), (0,)), ((), ())), preferred_element_type=F32,
        )

    def keep(value, low, high):
        for c in range(3):
            waves[c, low:high, :] = value[low:high, 128 * c : 128 * c + 128]

    def send_anomalies(u):
        @pl.loop(0, 4)
        def _(t):
            v = [
                jnp.concatenate([waves[c, pl.ds(8 * t + i, 8, stride=32), :] for i in range(8)], axis=0)
                for c in range(3)
            ]
            for c, value in enumerate(centred(v)):
                anom_out[u, pl.ds(8 * t, 8), :, 128 * c : 128 * c + 128] = value.astype(BF16).reshape(8, 8, 128)

        over_lat(anom_out.at[u], anom_in.at[u], sem_a + u)

    def lev_copy(u, to):
        return pltpu.make_async_remote_copy(
            anom_in.at[u, pl.ds(share * to, share)], mixed.at[u, zed], send_sem.at[sem_z + u], recv_sem.at[sem_z + u],
            device_id={"lev": to}, device_id_type=MESH,
        )

    def over_lev(u):
        lat_copy(anom_out.at[u], anom_in.at[u], sem_a + u).wait_recv()

        @pl.loop(1, levs)
        def _(k):
            lev_copy(u, (zed + k) % levs).start()

        mixed[u, zed] = anom_in[u, pl.ds(share * zed, share)]

    def lev_wait(u):
        return pltpu.make_async_remote_copy(
            mixed.at[u, pl.ds(0, levs - 1)], mixed.at[u, pl.ds(0, levs - 1)], send_sem.at[sem_z + u], recv_sem.at[sem_z + u],
            device_id={"lev": (zed + 1) % levs}, device_id_type=MESH,
        )

    for g in range(4):
        lat_copy(spec.at[g], spec_in.at[g], sem_s + g).wait_recv()
        if g == 0:
            keep(transform(0, 0, 0), 0, 256)
            send_anomalies(0)
            keep(transform(4, 0, 1), 0, 256)
            send_anomalies(4)
        else:
            keep(transform(g, g, 0), 32 * g, 256)
            keep(transform(g, g, 1), 0, 32 * g)
            send_anomalies(g)
        if g == 1:
            over_lev(0)
            over_lev(4)
        elif g > 1:
            over_lev(g - 1)
    over_lev(3)

    group = lax.broadcasted_iota(jnp.int32, (32, 128), 1) // 16
    for u in UNIT_ORDER:
        lev_wait(u).wait_recv()
        for j in range(3):
            v = [mixed[u, z, :, :, 128 * j : 128 * j + 128].astype(F32).reshape(32, 128) for z in range(8)]
            for bit in (1, 2, 4):
                high = (group // bit) % 2 == 1
                w = list(v)
                for i in range(8):
                    if i // bit % 2 == 0:
                        w[i] = jnp.where(high, pltpu.roll(v[i + bit], 16 * bit, 1), v[i])
                        w[i + bit] = jnp.where(high, v[i + bit], pltpu.roll(v[i], 128 - 16 * bit, 1))
                v = w
            for x in range(8):
                swapped[pl.ds(((u * 3 + j) * 8 + x) * 32, 32), :] = v[x]

    for b in range(8):
        rows = [(u, b) for u in range(min(b, 4) + 1)] + [(u, b - 8 + u) for u in range(max(1, 8 - b), 4)]
        x = jnp.concatenate([swapped[pl.ds(u * 768 + r, 96, stride=8), :] for u, r in rows], axis=0).astype(BF16)
        gram = lax.dot_general(x, x, (((0,), (0,)), ((), ())), preferred_element_type=F32)
        part_out[:, b] = gram.astype(BF16).reshape(8, 16, 128)

    @pl.loop(1, levs)
    def _(k):
        to = (zed + k) % levs
        pltpu.make_async_remote_copy(
            part_out.at[to], part_in.at[zed], send_sem.at[sem_p], recv_sem.at[sem_p],
            device_id={"lev": to}, device_id_type=MESH,
        ).start()

    part_in[zed] = part_out[zed]
    part_wait = pltpu.make_async_remote_copy(
        part_out.at[pl.ds(0, levs - 1)], part_in.at[pl.ds(0, levs - 1)], send_sem.at[sem_p], recv_sem.at[sem_p],
        device_id={"lev": (zed + 1) % levs}, device_id_type=MESH,
    )
    part_wait.wait_recv()
    for b in range(8):
        total = part_in[0, b].astype(F32)
        for z in range(1, 8):
            total += part_in[z, b].astype(F32)
        cov[b] = total / (11 * (2 * (32 * b + me) + 2)).astype(F32)

    def choose(d, start):
        n = start + (me + 512 - start) % 32
        own_out[d] = cov[jnp.minimum(n // 32, 7)]
        return start + counts[d]

    lax.fori_loop(0, lats, choose, jnp.int32(0))
    over_lat(own_out, own_in, sem_o)
    start = lax.fori_loop(0, lats, lambda d, t: t + jnp.where(d < me, counts[d], 0), jnp.int32(0))
    live = jnp.broadcast_to(counts[me], (16, 128))
    lat_copy(own_out, own_in, sem_o).wait_recv()
    for j in range(16):
        value = own_in[(start + j) % 32]
        out[j] = jnp.where(live > j, value, 0.0)

    lat_copy(leg_out, leg_in, sem_l).wait_send()
    for g in range(4):
        lat_copy(spec.at[g], spec_in.at[g], sem_s + g).wait_send()
    for u in range(UNITS):
        lat_copy(anom_out.at[u], anom_in.at[u], sem_a + u).wait_send()
        lev_wait(u).wait_send()
    part_wait.wait_send()
    lat_copy(own_out, own_in, sem_o).wait_send()


def fourier_tables():
    x = np.arange(512)
    a = np.array([a for pair in PAIRS for a in pair])
    tables = []
    for parity in range(2):
        m = (32 * a[:, None] + 2 * np.arange(16)[None, :] + parity).reshape(-1)
        angle = 2.0 * np.pi * ((m[:, None] * x[None]) % 1024) / 1024
        exact = np.concatenate([np.cos(angle), -np.sin(angle)]) / 32.0
        high = exact.astype(jnp.bfloat16)
        low = (exact - high.astype(np.float64)).astype(jnp.bfloat16)
        tables.append(np.concatenate([high, low], axis=1))
    return np.stack(tables)


def on_device(fields, legendre, owner_counts):
    vmem = pl.BlockSpec(memory_space=pltpu.VMEM)
    anywhere = pl.BlockSpec(memory_space=pl.ANY)
    return pl.pallas_call(
        kernel,
        out_shape=jax.ShapeDtypeStruct((16, 16, 128), F32),
        in_specs=[anywhere, anywhere, vmem, pl.BlockSpec(memory_space=pltpu.SMEM)],
        out_specs=vmem,
        scratch_shapes=[
            pltpu.VMEM((8, 1536, 128), F32),
            pltpu.VMEM((2, 256, 1024), BF16),
            pltpu.VMEM((3, 2048, 128), F32),
            pltpu.VMEM((4, 32, 2, 8, 384), BF16),
            pltpu.VMEM((32, UNITS, 8, 256), BF16),
            pltpu.VMEM((32, UNITS, 8, 256), BF16),
            pltpu.VMEM((4, 32, 2, 8, 384), BF16),
            pltpu.VMEM((2, 256, 128), F32),
            pltpu.VMEM((3, 256, 128), F32),
            pltpu.VMEM((UNITS, 32, 8, 384), BF16),
            pltpu.VMEM((UNITS, 32, 8, 384), BF16),
            pltpu.VMEM((UNITS, 8, 4, 8, 384), BF16),
            pltpu.VMEM((UNITS * 768, 128), F32),
            pltpu.VMEM((8, 8, 16, 128), BF16),
            pltpu.VMEM((8, 8, 16, 128), BF16),
            pltpu.VMEM((8, 16, 128), F32),
            pltpu.VMEM((32, 16, 128), F32),
            pltpu.VMEM((32, 16, 128), F32),
            pltpu.SemaphoreType.DMA((17,)),
            pltpu.SemaphoreType.DMA((17,)),
            pltpu.SemaphoreType.DMA((9,)),
        ],
        compiler_params=pltpu.CompilerParams(
            collective_id=0, has_side_effects=True, vmem_limit_bytes=48 * 2**20
        ),
        name="exchange",
    )(fields.reshape(1536, 1024), jnp.asarray(fourier_tables()), legendre, owner_counts)


def solution(mesh):
    return jax.shard_map(
        on_device,
        mesh=mesh,
        in_specs=(P(None, "lev", "lat", None), P("lat", None, None), P()),
        out_specs=P("lat", "lev", None),
        check_vma=False,
    )
```

```python
import functools

import jax
import jax.numpy as jnp
import numpy as np
from jax import lax
from jax.experimental import pallas as pl
from jax.experimental.pallas import tpu as pltpu
from jax.sharding import PartitionSpec as P

MESH = pl.DeviceIdType.MESH
F32, BF16 = jnp.float32, jnp.bfloat16
PAIRS = ((0, 4), (1, 7), (2, 6), (3, 5))
UNITS = 5
UNIT_ORDER = (0, 4, 1, 2, 3)


def centred(v):
    lane = lax.broadcasted_iota(jnp.int32, v[0].shape, 1)

    def whole(t):
        for shift in (64, 32, 16):
            t = t + pltpu.roll(t, shift, 1)
        return t

    t = v[1]
    for shift in (16, 32):
        t = t + jnp.where((lane // shift) % 2 == 0, pltpu.roll(t, 128 - shift, 1), pltpu.roll(t, shift, 1))
    other = pltpu.roll(t, 64, 1)
    real = (whole(v[0]) + jnp.where(lane < 64, t, other)) * (1.0 / 12.0)
    imag = (whole(v[2]) + jnp.where(lane < 64, other, t)) * (1.0 / 12.0)
    return v[0] - real, v[1] - jnp.where(lane < 64, real, imag), v[2] - imag


def kernel(
    fields, tables, leg_hbm, counts_hbm, out,
    leg, counts, grid, table, spectra, spec, leg_out, leg_in, spec_in, packed, waves, anom_out, anom_in, mixed, swapped, total, part_out, part_in, cov, own_out, own_in,
    send_sem, recv_sem, load_sem,
):
    me, zed = lax.axis_index("lat"), lax.axis_index("lev")
    lats, levs = 32, 8
    share = lats // levs
    sem_l, sem_s, sem_a, sem_z, sem_p, sem_o = 0, 1, 5, 10, 15, 17
    sent, arriving = [], {}

    load_leg = pltpu.make_async_copy(leg_hbm, leg, load_sem.at[9])
    load_leg.start()
    loads = [pltpu.make_async_copy(tables, table, load_sem.at[8]), pltpu.make_async_copy(counts_hbm, counts, load_sem.at[10])] + [
        pltpu.make_async_copy(fields.at[:, pl.ds(128 * c, 128)], grid.at[c], load_sem.at[c]) for c in range(8)
    ]
    for load in loads:
        load.start()
    chips_y = [(me // 8 + d) % 4 for d in range(4)]
    chips_x = [(me // 2 + d) % 4 for d in range(4)]
    cores = [me % 2, 1 - me % 2]
    chips = [4 * chips_y[(i // 4 + i) % 4] + chips_x[i % 4] for i in range(16)]
    partners = [(2 * chips[k // 2] + cores[k % 2], chips[k // 2] + 16 * cores[k % 2]) for k in range(32)]
    planes = [(zed + k) % levs for k in (1, 7, 2, 6, 3, 5, 4)]

    barrier = pltpu.get_barrier_semaphore()
    for to, _ in partners[1:]:
        pl.semaphore_signal(barrier, inc=1, device_id={"lat": to}, device_id_type=MESH)
    for to in planes:
        pl.semaphore_signal(barrier, inc=1, device_id={"lev": to}, device_id_type=MESH)

    def over_lat(source, target, sem, halves=False):
        for to, half in partners[1:]:
            pltpu.make_async_remote_copy(
                source.at[half if halves else to], target.at[me], send_sem.at[sem], recv_sem.at[sem],
                device_id={"lat": to}, device_id_type=MESH,
            ).start()
        target[me] = source[partners[0][1] if halves else me]
        arriving[sem] = pltpu.make_async_remote_copy(
            source.at[pl.ds(0, lats - 1)], target.at[pl.ds(0, lats - 1)], send_sem.at[sem], recv_sem.at[sem],
            device_id={"lat": partners[1][0]}, device_id_type=MESH,
        )
        sent.append(arriving[sem])

    load_leg.wait()
    column = lax.broadcasted_iota(jnp.int32, (32, 256), 1)
    for u in range(UNITS):
        for j in range(8):
            rows = leg[j, 32 * u : 32 * u + 32, :].astype(F32)
            if 0 < u < 4:
                other = leg[j, 32 * (8 - u) : 32 * (8 - u) + 32, :].astype(F32)
                rows = jnp.where(column < 32 * u, pltpu.roll(other, 32 * u, 1), rows)
            elif u == 4:
                rows = jnp.where(column < 128, 0.0, rows)
            for c in range(2):
                packed[c, pl.ds(j, 32, stride=8), :] = rows[:, 128 * c : 128 * c + 128]
        for c in range(2):
            leg_out[:, u, :, 128 * c : 128 * c + 128] = packed[c].astype(BF16).reshape(32, 8, 128)

    pl.semaphore_wait(barrier, lats - 1 + levs - 1)
    over_lat(leg_out, leg_in, sem_l)
    for load in loads:
        load.wait()

    lane = lax.broadcasted_iota(jnp.int32, (128, 128), 1)

    @pl.loop(0, 8)
    def _(j):
        for p in range(2):
            high, low = [], []
            for c in range(4):
                first = grid[c, pl.ds(j, 192, stride=8), :]
                second = grid[c + 4, pl.ds(j, 192, stride=8), :]
                value = first + second if p == 0 else first - second
                high.append(value.astype(BF16))
                low.append((value - high[-1].astype(F32)).astype(BF16))
            right = jnp.concatenate(high + low + high, axis=1)
            right = jnp.concatenate([right, jnp.zeros((64, 1536), BF16)], axis=0)
            left = jnp.concatenate([table[p, :, :512], table[p, :, :512], table[p, :, 512:]], axis=1)
            sums = lax.dot_general(left, right, (((1,), (1,)), ((), ())), preferred_element_type=F32)
            rows = pl.ds(1024 * p + j, 128, stride=8)
            spectra[0, rows, :] = sums[:128, :128]
            spectra[1, rows, :] = jnp.where(lane < 64, sums[:128, 128:], pltpu.roll(sums[128:, 128:], 64, 1))
            spectra[2, rows, :] = sums[128:, :128]

    def send_spectra(g):
        for aa in range(2):
            for p in range(2):
                for c in range(3):
                    value = spectra[c, pl.ds(1024 * p + 128 * (2 * g + aa), 128), :].astype(BF16)
                    spec[g, 16 * p : 16 * p + 16, aa, :, 128 * c : 128 * c + 128] = value.reshape(16, 8, 128)
        over_lat(spec.at[g], spec_in.at[g], sem_s + g, halves=True)

    send_spectra(0)
    send_spectra(1)
    arriving.pop(sem_l).wait_recv()

    def transform(u, g, aa):
        return lax.dot_general(
            leg_in[:, u].reshape(256, 256), spec_in[g, :, aa].reshape(256, 384),
            (((0,), (0,)), ((), ())), preferred_element_type=F32,
        )

    def keep(value, low, high):
        for c in range(3):
            waves[c, low:high, :] = value[low:high, 128 * c : 128 * c + 128]

    def send_anomalies(u):
        @pl.loop(0, 4)
        def _(t):
            v = [
                jnp.concatenate([waves[c, pl.ds(8 * t + i, 8, stride=32), :] for i in range(8)], axis=0)
                for c in range(3)
            ]
            for c, value in enumerate(centred(v)):
                anom_out[u, pl.ds(8 * t, 8), :, 128 * c : 128 * c + 128] = value.astype(BF16).reshape(8, 8, 128)

        over_lat(anom_out.at[u], anom_in.at[u], sem_a + u)

    def over_lev(source, target, sem):
        for to in planes:
            pltpu.make_async_remote_copy(
                source(to), target(zed), send_sem.at[sem], recv_sem.at[sem],
                device_id={"lev": to}, device_id_type=MESH,
            ).start()
        target(zed)[...] = source(zed)[...]
        arriving[sem] = pltpu.make_async_remote_copy(
            target(pl.ds(0, levs - 1)), target(pl.ds(0, levs - 1)), send_sem.at[sem], recv_sem.at[sem],
            device_id={"lev": planes[0]}, device_id_type=MESH,
        )
        sent.append(arriving[sem])

    def mix(u):
        arriving.pop(sem_a + u).wait_recv()
        over_lev(lambda to: anom_in.at[u, pl.ds(share * to, share)], lambda z: mixed.at[u, z], sem_z + u)

    for g in range(4):
        arriving.pop(sem_s + g).wait_recv()
        if g == 0:
            keep(transform(0, 0, 0), 0, 256)
            send_anomalies(0)
            keep(transform(4, 0, 1), 0, 256)
            send_anomalies(4)
        else:
            keep(transform(g, g, 0), 32 * g, 256)
            keep(transform(g, g, 1), 0, 32 * g)
            send_anomalies(g)
        if g < 2:
            send_spectra(g + 2)
        if g == 1:
            mix(0)
            mix(4)
        elif g > 1:
            mix(g - 1)
    mix(3)

    group = lax.broadcasted_iota(jnp.int32, (32, 128), 1) // 16

    def swap(u):
        arriving.pop(sem_z + u).wait_recv()
        for j in range(3):
            v = [mixed[u, z, :, :, 128 * j : 128 * j + 128].astype(F32).reshape(32, 128) for z in range(8)]
            for bit in (1, 2, 4):
                high = (group // bit) % 2 == 1
                w = list(v)
                for i in range(8):
                    if i // bit % 2 == 0:
                        w[i] = jnp.where(high, pltpu.roll(v[i + bit], 16 * bit, 1), v[i])
                        w[i + bit] = jnp.where(high, v[i + bit], pltpu.roll(v[i], 128 - 16 * bit, 1))
                v = w
            for x in range(8):
                swapped[pl.ds(((u * 3 + j) * 8 + x) * 32, 32), :] = v[x]

    def gram(b, units):
        rows = [(u, b) for u in range(min(b, 4) + 1)] + [(u, b - 8 + u) for u in range(max(1, 8 - b), 4)]
        x = [swapped[pl.ds(u * 768 + r, 96, stride=8), :] for u, r in rows if u in units]
        x = jnp.concatenate(x, axis=0).astype(BF16)
        return lax.dot_general(x, x, (((0,), (0,)), ((), ())), preferred_element_type=F32)

    def reduce(sem, low, high):
        over_lev(
            lambda to: part_out.at[pl.ds(low, high - low), to], lambda z: part_in.at[pl.ds(low, high - low), z], sem
        )

    for u in (0, 4, 1, 2):
        swap(u)
    for b in range(8):
        value = gram(b, (0, 4, 1, 2))
        if b < 3:
            part_out[b] = value.astype(BF16).reshape(8, 16, 128)
        else:
            total[b] = value
        if b == 2:
            reduce(sem_p, 0, 3)
    swap(3)
    for b in range(3, 8):
        part_out[b] = (total[b] + gram(b, (3,))).astype(BF16).reshape(8, 16, 128)
    reduce(sem_p + 1, 3, 8)
    arriving.pop(sem_p).wait_recv()
    for b in range(8):
        if b == 3:
            arriving.pop(sem_p + 1).wait_recv()
        value = part_in[b, 0].astype(F32)
        for z in range(1, 8):
            value += part_in[b, z].astype(F32)
        cov[b] = value / (11 * (2 * (32 * b + me) + 2)).astype(F32)

    def choose(d, start):
        n = start + (me + 512 - start) % 32
        own_out[d] = cov[jnp.minimum(n // 32, 7)]
        return start + counts[d]

    lax.fori_loop(0, lats, choose, jnp.int32(0))
    over_lat(own_out, own_in, sem_o)
    start = lax.fori_loop(0, lats, lambda d, t: t + jnp.where(d < me, counts[d], 0), jnp.int32(0))
    live = jnp.broadcast_to(counts[me], (16, 128))
    arriving.pop(sem_o).wait_recv()
    for j in range(16):
        value = own_in[(start + j) % 32]
        out[j] = jnp.where(live > j, value, 0.0)

    for copy in sent:
        copy.wait_send()


def fourier_tables():
    x = np.arange(512)
    a = np.array([a for pair in PAIRS for a in pair])
    tables = []
    for parity in range(2):
        m = (32 * a[:, None] + 2 * np.arange(16)[None, :] + parity).reshape(-1)
        angle = 2.0 * np.pi * ((m[:, None] * x[None]) % 1024) / 1024
        exact = np.concatenate([np.cos(angle), -np.sin(angle)]) / 32.0
        high = exact.astype(jnp.bfloat16)
        low = (exact - high.astype(np.float64)).astype(jnp.bfloat16)
        tables.append(np.concatenate([high, low], axis=1))
    return np.stack(tables)


def on_device(fields, legendre, owner_counts):
    vmem = pl.BlockSpec(memory_space=pltpu.VMEM)
    anywhere = pl.BlockSpec(memory_space=pl.ANY)
    return pl.pallas_call(
        kernel,
        out_shape=jax.ShapeDtypeStruct((16, 16, 128), F32),
        in_specs=[anywhere] * 4,
        out_specs=vmem,
        scratch_shapes=[
            pltpu.VMEM((8, 256, 256), BF16),
            pltpu.SMEM((32,), jnp.int32),
            pltpu.VMEM((8, 1536, 128), F32),
            pltpu.VMEM((2, 256, 1024), BF16),
            pltpu.VMEM((3, 2048, 128), F32),
            pltpu.VMEM((4, 32, 2, 8, 384), BF16),
            pltpu.VMEM((32, UNITS, 8, 256), BF16),
            pltpu.VMEM((32, UNITS, 8, 256), BF16),
            pltpu.VMEM((4, 32, 2, 8, 384), BF16),
            pltpu.VMEM((2, 256, 128), F32),
            pltpu.VMEM((3, 256, 128), F32),
            pltpu.VMEM((UNITS, 32, 8, 384), BF16),
            pltpu.VMEM((UNITS, 32, 8, 384), BF16),
            pltpu.VMEM((UNITS, 8, 4, 8, 384), BF16),
            pltpu.VMEM((UNITS * 768, 128), F32),
            pltpu.VMEM((8, 128, 128), F32),
            pltpu.VMEM((8, 8, 16, 128), BF16),
            pltpu.VMEM((8, 8, 16, 128), BF16),
            pltpu.VMEM((8, 16, 128), F32),
            pltpu.VMEM((32, 16, 128), F32),
            pltpu.VMEM((32, 16, 128), F32),
            pltpu.SemaphoreType.DMA((18,)),
            pltpu.SemaphoreType.DMA((18,)),
            pltpu.SemaphoreType.DMA((11,)),
        ],
        compiler_params=pltpu.CompilerParams(
            collective_id=0, has_side_effects=True, vmem_limit_bytes=63 * 2**20
        ),
        name="exchange",
    )(fields.reshape(1536, 1024), jnp.asarray(fourier_tables()), legendre, owner_counts)


def solution(mesh):
    return jax.shard_map(
        on_device,
        mesh=mesh,
        in_specs=(P(None, "lev", "lat", None), P("lat", None, None), P()),
        out_specs=P("lat", "lev", None),
        check_vma=False,
    )
```

```python
import functools

import jax
import jax.numpy as jnp
import numpy as np
from jax import lax
from jax.experimental import pallas as pl
from jax.experimental.pallas import tpu as pltpu
from jax.sharding import PartitionSpec as P

MESH = pl.DeviceIdType.MESH
F32, BF16 = jnp.float32, jnp.bfloat16
UNITS = ((0,), (1, 7), (2, 6), (3, 5), (4,))


def centred(v):
    lane = lax.broadcasted_iota(jnp.int32, v[0].shape, 1)

    def whole(t):
        for shift in (64, 32, 16):
            t = t + pltpu.roll(t, shift, 1)
        return t

    t = v[1]
    for shift in (16, 32):
        t = t + jnp.where((lane // shift) % 2 == 0, pltpu.roll(t, 128 - shift, 1), pltpu.roll(t, shift, 1))
    other = pltpu.roll(t, 64, 1)
    real = (whole(v[0]) + jnp.where(lane < 64, t, other)) * (1.0 / 12.0)
    imag = (whole(v[2]) + jnp.where(lane < 64, other, t)) * (1.0 / 12.0)
    return v[0] - real, v[1] - jnp.where(lane < 64, real, imag), v[2] - imag


def kernel(
    fields, tables, leg_hbm, counts_hbm, out,
    leg, counts, grid, table, spectra, spec_one, spec_two, leg_out, leg_half, leg_in, half_leg_in, into_one, into_two, packed, waves,
    anom_out, anom_half, anom_in, half_in, mixed, mixed_half, swapped, total, part_out, part_in, cov, own_out, own_in,
    send_sem, recv_sem, load_sem,
):
    me, zed = lax.axis_index("lat"), lax.axis_index("lev")
    lats, levs = 32, 8
    share = lats // levs
    sem_l, sem_s, sem_a, sem_z, sem_p, sem_o = 0, 3, 8, 13, 18, 20
    sent, arriving = [], {}
    spec = [(spec_one, (0,)), (spec_two, (0,)), (spec_two, (1,)), (spec_two, (2,)), (spec_one, (1,))]
    spec_in = [(into_one, (0,)), (into_two, (0,)), (into_two, (1,)), (into_two, (2,)), (into_one, (1,))]
    anomalies = [(anom_out, (u,)) for u in range(4)] + [(anom_half, ())]
    received = [(anom_in, (u,)) for u in range(4)] + [(half_in, ())]
    levels = [(mixed, (u,)) for u in range(4)] + [(mixed_half, ())]

    def view(part, index):
        ref, lead = part
        return ref.at[(*lead, index)]

    def read(part, *index):
        ref, lead = part
        return ref[(*lead, *index)]

    def store(part, value, *index):
        ref, lead = part
        ref[(*lead, *index)] = value

    every = slice(None)

    load_leg = pltpu.make_async_copy(leg_hbm, leg, load_sem.at[9])
    load_leg.start()
    loads = [pltpu.make_async_copy(tables, table, load_sem.at[8]), pltpu.make_async_copy(counts_hbm, counts, load_sem.at[10])] + [
        pltpu.make_async_copy(fields.at[:, pl.ds(128 * c, 128)], grid.at[c], load_sem.at[c]) for c in range(8)
    ]
    for load in loads:
        load.start()
    chips_y = [(me // 8 + d) % 4 for d in range(4)]
    chips_x = [(me // 2 + d) % 4 for d in range(4)]
    cores = [me % 2, 1 - me % 2]
    chips = [4 * chips_y[(i // 4 + i) % 4] + chips_x[i % 4] for i in range(16)]
    partners = [(2 * chips[k % 16] + cores[k // 16], chips[k % 16] + 16 * cores[k // 16]) for k in range(32)]
    planes = [(zed + k) % levs for k in (1, 7, 2, 6, 3, 5, 4)]

    barrier = pltpu.get_barrier_semaphore()
    for to, _ in partners[1:]:
        pl.semaphore_signal(barrier, inc=1, device_id={"lat": to}, device_id_type=MESH)
    for to in planes:
        pl.semaphore_signal(barrier, inc=1, device_id={"lev": to}, device_id_type=MESH)

    def over_lat(source, target, sem, halves=False):
        for to, half in partners[1:]:
            pltpu.make_async_remote_copy(
                view(source, half if halves else to), view(target, me), send_sem.at[sem], recv_sem.at[sem],
                device_id={"lat": to}, device_id_type=MESH,
            ).start()
        store(target, read(source, partners[0][1] if halves else me), me)
        arriving[sem] = pltpu.make_async_remote_copy(
            view(source, pl.ds(0, lats - 1)), view(target, pl.ds(0, lats - 1)), send_sem.at[sem], recv_sem.at[sem],
            device_id={"lat": partners[1][0]}, device_id_type=MESH,
        )
        sent.append(arriving[sem])

    load_leg.wait()
    column = lax.broadcasted_iota(jnp.int32, (32, 256), 1)
    for u in range(len(UNITS)):
        for j in range(8):
            rows = leg[j, 32 * u : 32 * u + 32, :].astype(F32)
            if 0 < u < 4:
                other = leg[j, 32 * (8 - u) : 32 * (8 - u) + 32, :].astype(F32)
                rows = jnp.where(column < 32 * u, pltpu.roll(other, 32 * u, 1), rows)
            for c in range(2):
                packed[c, pl.ds(j, 32, stride=8), :] = rows[:, 128 * c : 128 * c + 128]
        if u == 4:
            leg_half[...] = packed[1].astype(BF16).reshape(32, 8, 128)
        else:
            for c in range(2):
                leg_out[:, u, :, 128 * c : 128 * c + 128] = packed[c].astype(BF16).reshape(32, 8, 128)

    pl.semaphore_wait(barrier, lats - 1 + levs - 1)
    over_lat((leg_out, ()), (leg_in, ()), sem_l)
    for load in loads:
        load.wait()

    lane = lax.broadcasted_iota(jnp.int32, (128, 128), 1)

    @pl.loop(0, 8, unroll=2)
    def _(j):
        for p in range(2):
            high, low = [], []
            for c in range(4):
                first = grid[c, pl.ds(j, 192, stride=8), :]
                second = grid[c + 4, pl.ds(j, 192, stride=8), :]
                value = first + second if p == 0 else first - second
                high.append(value.astype(BF16))
                low.append((value - high[-1].astype(F32)).astype(BF16))
            right = jnp.concatenate(high + low + high, axis=1)
            right = jnp.concatenate([right, jnp.zeros((64, 1536), BF16)], axis=0)
            left = jnp.concatenate([table[p, :, :512], table[p, :, :512], table[p, :, 512:]], axis=1)
            sums = lax.dot_general(left, right, (((1,), (1,)), ((), ())), preferred_element_type=F32)
            rows = pl.ds(1024 * p + j, 128, stride=8)
            spectra[0, rows, :] = sums[:128, :128]
            spectra[1, rows, :] = jnp.where(lane < 64, sums[:128, 128:], pltpu.roll(sums[128:, 128:], 64, 1))
            spectra[2, rows, :] = sums[128:, :128]

    def send_spectra(u):
        first = sum(len(unit) for unit in UNITS[:u])
        for aa in range(len(UNITS[u])):
            for p in range(2):
                for c in range(3):
                    value = spectra[c, pl.ds(1024 * p + 128 * (first + aa), 128), :].astype(BF16)
                    value = value.reshape(16, 8, 128)
                    store(spec[u], value, pl.ds(16 * p, 16), aa, every, pl.ds(128 * c, 128))
        over_lat(spec[u], spec_in[u], sem_s + u, halves=True)

    send_spectra(0)
    send_spectra(1)
    over_lat((leg_half, ()), (half_leg_in, ()), sem_l + 2)
    arriving.pop(sem_l).wait_recv()

    def transform(u, aa):
        weights = half_leg_in[...].reshape(256, 128) if u == 4 else leg_in[:, u].reshape(256, 256)
        if aa == 1:
            weights = weights[:, :128]
        return lax.dot_general(
            weights, read(spec_in[u], every, aa).reshape(256, 384), (((0,), (0,)), ((), ())), preferred_element_type=F32
        )

    def keep(value, low, high):
        for c in range(3):
            waves[c, low:high, :] = value[low:high, 128 * c : 128 * c + 128]

    def send_anomalies(u):
        if u == 4:
            arriving.pop(sem_l + 2).wait_recv()
        arriving.pop(sem_s + u).wait_recv()
        if u < 4:
            keep(transform(u, 0), 32 * u, 256)
            if u > 0:
                keep(transform(u, 1), 0, 32 * u)
        else:
            value = transform(u, 0)
            v = centred([value[:, 128 * c : 128 * c + 128] for c in range(3)])
            waves[0, :128, :] = v[0]
            waves[0, 128:, :] = v[1]
            waves[1, :128, :] = v[2]

        @pl.loop(0, 4)
        def _(t):
            v = [
                jnp.concatenate([waves[c, pl.ds(8 * t + i, 8, stride=32), :] for i in range(8)], axis=0)
                for c in range(3 if u < 4 else 2)
            ]
            for c, value in enumerate(centred(v) if u < 4 else v):
                value = value.astype(BF16).reshape(8, 8, 128)
                store(anomalies[u], value, pl.ds(8 * t, 8), every, pl.ds(128 * c, 128))

        over_lat(anomalies[u], received[u], sem_a + u)

    def over_lev(source, target, sem):
        for to in planes:
            pltpu.make_async_remote_copy(
                source(to), target(zed), send_sem.at[sem], recv_sem.at[sem],
                device_id={"lev": to}, device_id_type=MESH,
            ).start()
        target(zed)[...] = source(zed)[...]
        arriving[sem] = pltpu.make_async_remote_copy(
            target(pl.ds(0, levs - 1)), target(pl.ds(0, levs - 1)), send_sem.at[sem], recv_sem.at[sem],
            device_id={"lev": planes[0]}, device_id_type=MESH,
        )
        sent.append(arriving[sem])

    def mix(u):
        arriving.pop(sem_a + u).wait_recv()
        over_lev(lambda to: view(received[u], pl.ds(share * to, share)), lambda z: view(levels[u], z), sem_z + u)

    group = lax.broadcasted_iota(jnp.int32, (32, 128), 1) // 16

    def swap(u):
        arriving.pop(sem_z + u).wait_recv()
        for j in range(3 if u < 4 else 2):
            v = [read(levels[u], z, every, every, pl.ds(128 * j, 128)).astype(F32).reshape(32, 128) for z in range(8)]
            for bit in (1, 2, 4):
                high = (group // bit) % 2 == 1
                w = list(v)
                for i in range(8):
                    if i // bit % 2 == 0:
                        w[i] = jnp.where(high, pltpu.roll(v[i + bit], 16 * bit, 1), v[i])
                        w[i + bit] = jnp.where(high, v[i + bit], pltpu.roll(v[i], 128 - 16 * bit, 1))
                v = w
            for x in range(8):
                swapped[pl.ds(((u * 3 + j) * 8 + x) * 32, 32), :] = v[x]

    send_anomalies(0)
    send_spectra(2)
    send_anomalies(1)
    send_spectra(3)
    mix(0)
    send_anomalies(2)
    send_spectra(4)
    mix(1)
    send_anomalies(3)
    mix(2)
    swap(0)
    send_anomalies(4)
    swap(1)
    mix(3)
    swap(2)
    mix(4)

    def gram(b, units):
        x = []
        for u in units:
            if u < 4:
                rows = [b] * (b >= u) + [b - 8 + u] * (8 - u <= b < 8)
                x += [swapped[pl.ds(768 * u + r, 96, stride=8), :] for r in rows if 0 <= r and (u > 0 or r == b)]
            elif b >= 4:
                x += [swapped[pl.ds(3072 + r, 32, stride=8), :] for r in (b - 4, b, 256 + b - 4)]
        x = jnp.concatenate(x, axis=0).astype(BF16)
        return lax.dot_general(x, x, (((0,), (0,)), ((), ())), preferred_element_type=F32)

    def reduce(sem, low, high):
        over_lev(
            lambda to: part_out.at[pl.ds(low, high - low), to], lambda z: part_in.at[pl.ds(low, high - low), z], sem
        )

    for b in range(8):
        total[b] = gram(b, (0, 1, 2))
    swap(3)
    for b in range(8):
        value = total[b] + gram(b, (3,)) if b >= 3 else total[b]
        if b < 4:
            part_out[b] = value.astype(BF16).reshape(8, 16, 128)
        else:
            total[b] = value
        if b == 3:
            reduce(sem_p, 0, 4)
    swap(4)
    for b in range(4, 8):
        part_out[b] = (total[b] + gram(b, (4,))).astype(BF16).reshape(8, 16, 128)
    reduce(sem_p + 1, 4, 8)
    arriving.pop(sem_p).wait_recv()
    for b in range(8):
        if b == 4:
            arriving.pop(sem_p + 1).wait_recv()
        value = part_in[b, 0].astype(F32)
        for z in range(1, 8):
            value += part_in[b, z].astype(F32)
        cov[b] = value / (11 * (2 * (32 * b + me) + 2)).astype(F32)

    def choose(d, start):
        n = start + (me + 512 - start) % 32
        own_out[d] = cov[jnp.minimum(n // 32, 7)]
        return start + counts[d]

    lax.fori_loop(0, lats, choose, jnp.int32(0))
    over_lat((own_out, ()), (own_in, ()), sem_o)
    start = lax.fori_loop(0, lats, lambda d, t: t + jnp.where(d < me, counts[d], 0), jnp.int32(0))
    live = jnp.broadcast_to(counts[me], (16, 128))
    arriving.pop(sem_o).wait_recv()
    for j in range(16):
        value = own_in[(start + j) % 32]
        out[j] = jnp.where(live > j, value, 0.0)

    for copy in sent:
        copy.wait_send()


def fourier_tables():
    x = np.arange(512)
    a = np.array([a for unit in UNITS for a in unit])
    tables = []
    for parity in range(2):
        m = (32 * a[:, None] + 2 * np.arange(16)[None, :] + parity).reshape(-1)
        angle = 2.0 * np.pi * ((m[:, None] * x[None]) % 1024) / 1024
        exact = np.concatenate([np.cos(angle), -np.sin(angle)]) / 32.0
        high = exact.astype(jnp.bfloat16)
        low = (exact - high.astype(np.float64)).astype(jnp.bfloat16)
        tables.append(np.concatenate([high, low], axis=1))
    return np.stack(tables)


def on_device(fields, legendre, owner_counts):
    vmem = pl.BlockSpec(memory_space=pltpu.VMEM)
    hbm = pl.BlockSpec(memory_space=pltpu.HBM)
    return pl.pallas_call(
        kernel,
        out_shape=jax.ShapeDtypeStruct((16, 16, 128), F32),
        in_specs=[hbm] * 4,
        out_specs=vmem,
        scratch_shapes=[
            pltpu.VMEM((8, 256, 256), BF16),
            pltpu.SMEM((32,), jnp.int32),
            pltpu.VMEM((8, 1536, 128), F32),
            pltpu.VMEM((2, 256, 1024), BF16),
            pltpu.VMEM((3, 2048, 128), F32),
            pltpu.VMEM((2, 32, 1, 8, 384), BF16),
            pltpu.VMEM((3, 32, 2, 8, 384), BF16),
            pltpu.VMEM((32, 4, 8, 256), BF16),
            pltpu.VMEM((32, 8, 128), BF16),
            pltpu.VMEM((32, 4, 8, 256), BF16),
            pltpu.VMEM((32, 8, 128), BF16),
            pltpu.VMEM((2, 32, 1, 8, 384), BF16),
            pltpu.VMEM((3, 32, 2, 8, 384), BF16),
            pltpu.VMEM((2, 256, 128), F32),
            pltpu.VMEM((3, 256, 128), F32),
            pltpu.VMEM((4, 32, 8, 384), BF16),
            pltpu.VMEM((32, 8, 256), BF16),
            pltpu.VMEM((4, 32, 8, 384), BF16),
            pltpu.VMEM((32, 8, 256), BF16),
            pltpu.VMEM((4, 8, 4, 8, 384), BF16),
            pltpu.VMEM((8, 4, 8, 256), BF16),
            pltpu.VMEM((3584, 128), F32),
            pltpu.VMEM((8, 128, 128), F32),
            pltpu.VMEM((8, 8, 16, 128), BF16),
            pltpu.VMEM((8, 8, 16, 128), BF16),
            pltpu.VMEM((8, 16, 128), F32),
            pltpu.VMEM((32, 16, 128), F32),
            pltpu.VMEM((32, 16, 128), F32),
            pltpu.SemaphoreType.DMA((21,)),
            pltpu.SemaphoreType.DMA((21,)),
            pltpu.SemaphoreType.DMA((11,)),
        ],
        compiler_params=pltpu.CompilerParams(
            collective_id=0, has_side_effects=True, vmem_limit_bytes=56_000_000
        ),
        name="exchange",
    )(fields.reshape(1536, 1024), jnp.asarray(fourier_tables()), legendre, owner_counts)


def solution(mesh):
    return jax.shard_map(
        on_device,
        mesh=mesh,
        in_specs=(P(None, "lev", "lat", None), P("lat", None, None), P()),
        out_specs=P("lat", "lev", None),
        check_vma=False,
    )
```
